128 devices in a mesh: lat: 4 (over x_hi, core), lon: 4 (over z), lev: 8 (over y, x_lo).
Axes of the slice: x: 4 (x_hi: 2, x_lo: 2; x = x_hi * 2 + x_lo), y: 4, z: 4, core: 2. Of those that a mesh axis runs over, the one named last changes fastest.
Arguments:
- initial_heat: float32 [128, 512, 32, 128], P('lat', 'lon', 'lev'), may hold values from 0.5 to 2
- diffusivity_ratio: float32 [128, 512, 32, 128], P('lat', 'lon', 'lev'), may hold values from 0.03 to 0.15
- forcing_term: float32 [128, 512, 32, 128], P('lat', 'lon', 'lev'), may hold values from -0.2 to 0.2
Outputs:
- standard_deviation_score: float32 [128, 512, 32, 128], P('lat', 'lon', 'lev')
- temperature_end: float32 [128, 512, 32, 128], P('lat', 'lon', 'lev')
The draws below stay inside these ranges and needn't reach their ends.
All inputs are finite; a program needn't handle non-finite values.
Results may differ from the reference program's by a relative error of at most 0.00002.
Values sent between devices are 32-bit elements; how exact they have to be, the bound alone decides.
No kernel may reach another device: no remote copies, remote signals or barrier semaphores. Data moves between devices by JAX's collectives and lax.ppermute only.
A program may use at most 128 MiB of HBM per device.

```python
import jax
import jax.numpy as jnp
from jax import lax

GRID_DEPTH = 128
GRID_WIDTH = 512
GRID_HEIGHT = 32
MEMBER_TOTAL = 128
STEPS = 4


def steps_of(key, shape, cuts, least, top_value):
    level = 1.0
    for dim, shards_of in cuts:
        draws = jax.random.uniform(jax.random.fold_in(jax.random.fold_in(key, 6), dim), (shards_of,), jnp.float32, least / len(cuts), top_value / len(cuts))
        level = level * jnp.repeat(jnp.exp(draws), shape[dim] // shards_of).reshape((-1,) + (1,) * (len(shape) - 1 - dim))
    return level


def setup_inputs(seed: int = 0) -> dict:
    key_of = jax.random.split(jax.random.key(seed), 4)
    return {
        "initial_heat": jnp.clip(0.5 + 1.5 * jax.random.uniform(key_of[0], (GRID_DEPTH, GRID_WIDTH, GRID_HEIGHT, MEMBER_TOTAL), jnp.float32) ** steps_of(key_of[0], (GRID_DEPTH, GRID_WIDTH, GRID_HEIGHT, MEMBER_TOTAL), ((0, 4), (1, 4), (2, 8)), -0.2, 0.2), 0.5, 2.0),
        "diffusivity_ratio": jnp.clip(0.03 + 0.120000007 * jax.random.uniform(key_of[1], (GRID_DEPTH, GRID_WIDTH, GRID_HEIGHT, MEMBER_TOTAL), jnp.float32) ** steps_of(key_of[1], (GRID_DEPTH, GRID_WIDTH, GRID_HEIGHT, MEMBER_TOTAL), ((0, 4), (1, 4), (2, 8)), -0.2, 0.2), 0.03, 0.15),
        "forcing_term": jnp.clip(jax.random.uniform(key_of[2], (GRID_DEPTH, GRID_WIDTH, GRID_HEIGHT, MEMBER_TOTAL), jnp.float32, -0.2, 0.2) * steps_of(key_of[2], (GRID_DEPTH, GRID_WIDTH, GRID_HEIGHT, MEMBER_TOTAL), ((0, 4), (1, 4), (2, 8)), -0.4, 0.0), -0.2, 0.2),
    }


def without_rim(values, dims):
    for dim in dims:
        values = lax.slice_in_dim(values, 1, values.shape[dim] - 1, axis=dim)
    return values

def shifted_cells(values, dim, start, dims):
    others = [other for other in dims if other != dim]
    values = without_rim(values, others)
    return lax.slice_in_dim(values, start, start + values.shape[dim] - 2, axis=dim)

def march_forward(extended_grid_state, diffusivity_ratio, forcing_term):
    middle = without_rim(extended_grid_state, (0, 1, 2))
    lower = [shifted_cells(extended_grid_state, dim, 0, (0, 1, 2)) for dim in (0, 1, 2)]
    upper = [shifted_cells(extended_grid_state, dim, 2, (0, 1, 2)) for dim in (0, 1, 2)]
    spread = lower[0] + upper[0] + lower[1] + upper[1] + lower[2] + upper[2] - 6.0 * middle
    return middle + diffusivity_ratio * spread + forcing_term

def reference(initial_heat, diffusivity_ratio, forcing_term):
    for step in range(STEPS):
        initial_heat = march_forward(jnp.pad(initial_heat, ((1, 1), (1, 1), (1, 1), (0, 0)), mode='wrap'), diffusivity_ratio, forcing_term)
    row_mean_estimate = lax.optimization_barrier(jnp.mean(initial_heat, axis=1, keepdims=True))
    deviations_from_mean = initial_heat - row_mean_estimate
    line_variance = lax.optimization_barrier(jnp.mean(deviations_from_mean * deviations_from_mean, axis=1, keepdims=True))
    standard_deviation_score = deviations_from_mean * lax.rsqrt(line_variance + 0.0001)
    return (standard_deviation_score, initial_heat)
```

```python
import jax
import jax.numpy as jnp
from jax import lax
from jax.experimental import pallas as pl
from jax.experimental.pallas import tpu as pltpu
from jax.sharding import PartitionSpec as P

STEPS = 4
ROWS = 8


def shift(x, axis, by):
    size = lax.axis_size(axis)
    return lax.ppermute(x, axis, [(i, (i + by) % size) for i in range(size)])


def update_body(last, c, before, after, low, high, d, f, south, north, west, east, *outs):
    i = pl.program_id(0)
    n = pl.num_programs(0)
    out = outs[0]
    width = c.shape[1]
    place = lax.broadcasted_iota(jnp.int32, c.shape[1:], 0)
    first_row = jnp.where(i == 0, south[0], before[0])
    final_row = jnp.where(i == n - 1, north[0], after[0])
    for r in range(ROWS):
        x = c[r]
        lat_low = first_row if r == 0 else c[r - 1]
        lat_high = final_row if r == ROWS - 1 else c[r + 1]
        left = jnp.where(place == 0, west[0, r : r + 1, :], pltpu.roll(x, 1, 0))
        right = jnp.where(place == width - 1, east[0, r : r + 1, :], pltpu.roll(x, width - 1, 0))
        spread = lat_low + lat_high + left + right + low[r] + high[r] - 6.0 * x
        y = x + d[r] * spread + f[r]
        out[r] = y
        if last:
            total = jnp.sum(y, axis=0, keepdims=True)
            away = y - total * (1.0 / width)
            outs[1][r : r + 1, :] = total
            outs[2][r : r + 1, :] = jnp.sum(away * away, axis=0, keepdims=True)


def update(c, low, high, d, f, sides, k, last=False):
    south, north, west, east = sides
    depth, width, lanes = c.shape
    block = pl.BlockSpec((ROWS, width, lanes), lambda i: (i, 0, 0))
    row_before = pl.BlockSpec((1, width, lanes), lambda i: (jnp.maximum(i * ROWS - 1, 0), 0, 0))
    row_after = pl.BlockSpec((1, width, lanes), lambda i: (jnp.minimum(i * ROWS + ROWS, depth - 1), 0, 0))
    lat_edge = pl.BlockSpec((1, width, lanes), lambda i: (k, 0, 0))
    lon_edge = pl.BlockSpec((1, ROWS, lanes), lambda i: (k, i, 0))
    stat = pl.BlockSpec((ROWS, lanes), lambda i: (i, 0))
    shapes = [jax.ShapeDtypeStruct(c.shape, c.dtype)]
    specs = [block]
    if last:
        shapes += [jax.ShapeDtypeStruct((depth, lanes), c.dtype)] * 2
        specs += [stat] * 2
    got = pl.pallas_call(
        lambda *refs: update_body(last, *refs),
        grid=(depth // ROWS,),
        in_specs=[block, row_before, row_after, block, block, block, block, lat_edge, lat_edge, lon_edge, lon_edge],
        out_specs=specs,
        out_shape=shapes,
        compiler_params=pltpu.CompilerParams(vmem_limit_bytes=16 * 2**20),
        cost_estimate=pl.CostEstimate(flops=10 * c.size, bytes_accessed=6 * 4 * c.size, transcendentals=0),
        name="update",
    )(c, c, c, low, high, d, f, south, north, west, east)
    return got if last else got[0]


def sides_of(planes):
    def cut(take):
        return jnp.stack([take(p) for p in planes])

    return (
        shift(cut(lambda p: p[-1]), "lat", 1),
        shift(cut(lambda p: p[0]), "lat", -1),
        shift(cut(lambda p: p[:, -1]), "lon", 1),
        shift(cut(lambda p: p[:, 0]), "lon", -1),
    )


def finish_body(count, *refs):
    planes, stats, (score, end) = refs[:4], refs[4:-2], refs[-2:]
    width = planes[0].shape[1]
    for z in range(4):
        group, k = (0, 0) if z == 0 else (1, z - 1)
        sums = [stats[4 * group + j][k] for j in range(4)]
        powers = [stats[4 * group + j][k + (1 if group == 0 else 3)] for j in range(4)]
        mean = (sums[0] + sums[1] + sums[2] + sums[3]) * (1.0 / count)
        power = powers[0] + powers[1] + powers[2] + powers[3]
        for s in sums:
            gap = s * (1.0 / width) - mean
            power = power + width * (gap * gap)
        scale = lax.rsqrt(power * (1.0 / count) + 0.0001)
        for r in range(ROWS):
            y = planes[z][r]
            end[r, pl.ds(z, width, stride=4), :] = y
            score[r, pl.ds(z, width, stride=4), :] = (y - mean[r : r + 1, :]) * scale[r : r + 1, :]


def finish(planes, edge_stats, inner_stats):
    depth, width, lanes = planes[0].shape
    block = pl.BlockSpec((ROWS, width, lanes), lambda i: (i, 0, 0))
    wide = pl.BlockSpec((ROWS, 4 * width, lanes), lambda i: (i, 0, 0))
    edge = pl.BlockSpec((2, ROWS, lanes), lambda i: (0, i, 0))
    inner = pl.BlockSpec((6, ROWS, lanes), lambda i: (0, i, 0))
    count = width * lax.axis_size("lon")
    full = jax.ShapeDtypeStruct((depth, 4 * width, lanes), planes[0].dtype)
    score, end = pl.pallas_call(
        lambda *refs: finish_body(count, *refs),
        grid=(depth // ROWS,),
        in_specs=[block] * 4 + [edge] * 4 + [inner] * 4,
        out_specs=[wide] * 2,
        out_shape=[full] * 2,
        compiler_params=pltpu.CompilerParams(vmem_limit_bytes=24 * 2**20),
        cost_estimate=pl.CostEstimate(flops=20 * 4 * planes[0].size, bytes_accessed=12 * 4 * planes[0].size, transcendentals=0),
        name="finish",
    )(*planes, *edge_stats, *inner_stats)
    shape = (depth, width, 4, lanes)
    return score.reshape(shape), end.reshape(shape)


def from_all(x):
    return [x] + [shift(x, "lon", by) for by in (1, -1, 2)]


def local(initial_heat, diffusivity_ratio, forcing_term):
    u = [initial_heat[:, :, z, :] for z in range(4)]
    up = shift(u[3], "lev", 1)
    down = shift(u[0], "lev", -1)
    d = [diffusivity_ratio[:, :, z, :] for z in range(4)]
    f = [forcing_term[:, :, z, :] for z in range(4)]
    whole = sides_of(u)
    where = [(whole, z) for z in range(4)]
    for step in range(STEPS):
        last = step == STEPS - 1
        v = [None] * 4
        first, second = (0, 3) if step % 2 == 0 else (3, 0)
        halo = {0: up, 3: down}

        def advance(z):
            low = halo[0] if z == 0 else u[z - 1]
            high = halo[3] if z == 3 else u[z + 1]
            v[z] = update(u[z], low, high, d[z], f[z], *where[z], last=last)

        next_where = [None] * 4
        faces = {}
        advance(first)
        if not last:
            alone = sides_of([v[first]])
            next_where[first] = (alone, 0)
            faces[first] = shift(v[first], "lev", -1 if first == 0 else 1)
        advance(1)
        advance(2)
        advance(second)
        if not last:
            rest = [z for z in range(4) if z != first]
            together = sides_of([v[z] for z in rest])
            for k, z in enumerate(rest):
                next_where[z] = (together, k)
            faces[second] = shift(v[second], "lev", -1 if second == 0 else 1)
            up, down = faces[3], faces[0]
        u, where = v, next_where
    planes = [g[0] for g in u]
    inner = from_all(jnp.stack([u[z][1] for z in (1, 2, 3)] + [u[z][2] for z in (1, 2, 3)]))
    edge = from_all(jnp.stack([u[0][1], u[0][2]]))
    return finish(planes, edge, inner)


def solution(mesh):
    placed = P("lat", "lon", "lev", None)
    return jax.shard_map(
        local,
        mesh=mesh,
        in_specs=(placed,) * 3,
        out_specs=(placed, placed),
        check_vma=False,
    )
```

```python
import jax
import jax.numpy as jnp
from jax import lax
from jax.experimental import pallas as pl
from jax.experimental.pallas import tpu as pltpu
from jax.sharding import PartitionSpec as P


STEPS = 4
ROWS = 8


def shift(x, axis, by):
    size = lax.axis_size(axis)
    return lax.ppermute(x, axis, [(i, (i + by) % size) for i in range(size)])


def take_body(parts, whole, *refs):
    outs, sems = refs[:-1], refs[-1]
    copies = []
    for n, (out, part) in enumerate(zip(outs, parts)):
        copies += [
            pltpu.make_async_copy(source(whole), target(out), sems.at[n, k])
            for k, (source, target) in enumerate(part)
        ]
    for copy in copies:
        copy.start()
    for copy in copies:
        copy.wait()


def take(whole, shapes, parts):
    lanes = whole.shape[-1]
    got = pl.pallas_call(
        lambda *refs: take_body(parts, *refs),
        in_specs=[pl.BlockSpec(memory_space=pltpu.HBM)],
        out_specs=[pl.BlockSpec(memory_space=pltpu.VMEM)] * len(shapes),
        out_shape=[jax.ShapeDtypeStruct((*s, 1, lanes), whole.dtype) for s in shapes],
        scratch_shapes=[pltpu.SemaphoreType.DMA((len(parts), max(len(p) for p in parts)))],
        compiler_params=pltpu.CompilerParams(vmem_limit_bytes=2**20),
        cost_estimate=pl.CostEstimate(flops=20_000_000, bytes_accessed=2**22, transcendentals=0),
        name="take",
    )(whole)
    return [g.reshape(*s, lanes) for g, s in zip(got, shapes)]


def plane_of(z, depth, pieces):
    size = depth // pieces

    def piece(k):
        rows = pl.ds(k * size, size)
        return (lambda w: w.at[rows, :, z], lambda o: o.at[rows])

    return [piece(k) for k in range(pieces)]


def edge_of(pick):
    return [(lambda w, z=z: pick(w, z), lambda o, z=z: o.at[z]) for z in range(4)]


def grow_body(plan, last, *refs):
    zs, n_in, base = plan["zs"], plan["n_in"], plan["base"]
    ins, outs = refs[:n_in], refs[n_in:]
    i = pl.program_id(0)
    n = pl.num_programs(0)
    width = ins[0].shape[1]
    place = lax.broadcasted_iota(jnp.int32, ins[0].shape[1:], 0)
    for j, z in enumerate(zs):
        c, low, high, before, after, d, f, south, north, west, east = (ins[a] for a in plan[z])
        rest = outs[len(zs) :]

        @pl.loop(0, ROWS)
        def _(r, c=c, low=low, high=high, before=before, after=after, d=d, f=f, south=south, north=north, west=west, east=east, j=j):
            x = c[r]
            edge_low = jnp.where(i == 0, south[0], before[0])
            edge_high = jnp.where(i == n - 1, north[0], after[0])
            lat_low = jnp.where(r == 0, edge_low, c[jnp.maximum(r - 1, 0)])
            lat_high = jnp.where(r == ROWS - 1, edge_high, c[jnp.minimum(r + 1, ROWS - 1)])
            left = jnp.where(place == 0, west[0, pl.ds(r, 1), :], pltpu.roll(x, 1, 0))
            right = jnp.where(place == width - 1, east[0, pl.ds(r, 1), :], pltpu.roll(x, width - 1, 0))
            spread = lat_low + lat_high + left + right + low[r] + high[r] - 6.0 * x
            y = x + d[r] * spread + f[r]
            outs[j][r] = y
            if last:
                total = jnp.sum(y, axis=0, keepdims=True)
                away = y - total * (1.0 / width)
                rest[0][2 * j, pl.ds(r, 1), :] = total
                rest[0][2 * j + 1, pl.ds(r, 1), :] = jnp.sum(away * away, axis=0, keepdims=True)
            else:
                rest[2][base + j, pl.ds(r, 1), :] = y[width - 1 :, :]
                rest[3][base + j, pl.ds(r, 1), :] = y[:1, :]

        if not last:

            @pl.when(i == 0)
            def _(j=j):
                rest[1][base + j] = outs[j][0]

            @pl.when(i == n - 1)
            def _(j=j):
                rest[0][base + j] = outs[j][ROWS - 1]

    if plan["carried"]:
        held = [ins[a] for a in plan["carried"]]
        rest[2][:base] = held[2][...]
        rest[3][:base] = held[3][...]

        @pl.when(i == 0)
        def _():
            rest[0][:base] = held[0][...]
            rest[1][:base] = held[1][...]


def grow(zs, u, low, high, d, f, where, last, carried=()):
    depth, width, lanes = u[0].shape
    block = pl.BlockSpec((ROWS, width, lanes), lambda i: (i, 0, 0))
    row_before = pl.BlockSpec((1, width, lanes), lambda i: (jnp.maximum(i * ROWS - 1, 0), 0, 0))
    row_after = pl.BlockSpec((1, width, lanes), lambda i: (jnp.minimum(i * ROWS + ROWS, depth - 1), 0, 0))
    arrays, specs, seen = [], [], {}

    def use(key, array, spec):
        if key not in seen:
            seen[key] = len(arrays)
            arrays.append(array)
            specs.append(spec)
        return seen[key]

    plan = {"zs": zs}
    for z in zs:
        sides, k = where[z]
        lat_edge = pl.BlockSpec((1, width, lanes), lambda i, k=k: (k, 0, 0))
        lon_edge = pl.BlockSpec((1, ROWS, lanes), lambda i, k=k: (k, i, 0))
        plan[z] = [
            use(("u", z), u[z], block),
            use("low", low, block) if z == 0 else use(("u", z - 1), u[z - 1], block),
            use("high", high, block) if z == 3 else use(("u", z + 1), u[z + 1], block),
            use(("before", z), u[z], row_before),
            use(("after", z), u[z], row_after),
            use(("d", z), d[z], block),
            use(("f", z), f[z], block),
            use(("s", z), sides[0], lat_edge),
            use(("n", z), sides[1], lat_edge),
            use(("w", z), sides[2], lon_edge),
            use(("e", z), sides[3], lon_edge),
        ]
    m = len(zs)
    base = carried[0].shape[0] if carried else 0
    lat_all = pl.BlockSpec((base, width, lanes), lambda i: (0, 0, 0))
    lon_all = pl.BlockSpec((base, ROWS, lanes), lambda i: (0, i, 0))
    plan["carried"] = [
        use(("carried", k), a, spec) for k, (a, spec) in enumerate(zip(carried, (lat_all, lat_all, lon_all, lon_all)))
    ]
    plan["base"], plan["n_in"] = base, len(arrays)
    shapes, outs = [u[0].shape] * m, [block] * m
    if last:
        shapes += [(2 * m, depth, lanes)]
        outs += [pl.BlockSpec((2 * m, ROWS, lanes), lambda i: (0, i, 0))]
    else:
        t = base + m
        shapes += [(t, width, lanes)] * 2 + [(t, depth, lanes)] * 2
        outs += [pl.BlockSpec((t, width, lanes), lambda i: (0, 0, 0))] * 2
        outs += [pl.BlockSpec((t, ROWS, lanes), lambda i: (0, i, 0))] * 2
    got = pl.pallas_call(
        lambda *refs: grow_body(plan, last, *refs),
        grid=(depth // ROWS,),
        in_specs=specs,
        out_specs=outs,
        out_shape=[jax.ShapeDtypeStruct(s, u[0].dtype) for s in shapes],
        compiler_params=pltpu.CompilerParams(vmem_limit_bytes=(8 if m == 1 else 16) * 2**20),
        cost_estimate=pl.CostEstimate(flops=10_000_000 * m, bytes_accessed=2**22 * m, transcendentals=0),
        name="grow",
    )(*arrays)
    return got[:m], got[m:]


def exchange(south, north, east, west):
    return (
        shift(south, "lat", 1),
        shift(north, "lat", -1),
        shift(east, "lon", 1),
        shift(west, "lon", -1),
    )


def finish_body(count, *refs):
    planes, stats, (score, end) = refs[:4], refs[4:-2], refs[-2:]
    width = planes[0].shape[1]
    for z in range(4):
        group, k = (0, 0) if z == 0 else (1, 3 - z)
        sums = [stats[4 * group + j][2 * k] for j in range(4)]
        powers = [stats[4 * group + j][2 * k + 1] for j in range(4)]
        mean = (sums[0] + sums[1] + sums[2] + sums[3]) * (1.0 / count)
        power = powers[0] + powers[1] + powers[2] + powers[3]
        for s in sums:
            gap = s * (1.0 / width) - mean
            power = power + width * (gap * gap)
        scale = lax.rsqrt(power * (1.0 / count) + 0.0001)
        for r in range(ROWS):
            centre, factor = mean[r : r + 1, :], scale[r : r + 1, :]
            y = planes[z][r]
            end[r, pl.ds(z, width, stride=4), :] = y
            score[r, pl.ds(z, width, stride=4), :] = (y - centre) * factor


def finish(planes, edge_stats, inner_stats):
    depth, width, lanes = planes[0].shape
    block = pl.BlockSpec((ROWS, width, lanes), lambda i: (i, 0, 0))
    wide = pl.BlockSpec((ROWS, 4 * width, lanes), lambda i: (i, 0, 0))
    edge = pl.BlockSpec((2, ROWS, lanes), lambda i: (0, i, 0))
    inner = pl.BlockSpec((6, ROWS, lanes), lambda i: (0, i, 0))
    count = width * lax.axis_size("lon")
    full = jax.ShapeDtypeStruct((depth, 4 * width, lanes), planes[0].dtype)
    score, end = pl.pallas_call(
        lambda *refs: finish_body(count, *refs),
        grid=(depth // ROWS,),
        in_specs=[block] * 4 + [edge] * 4 + [inner] * 4,
        out_specs=[wide] * 2,
        out_shape=[full] * 2,
        compiler_params=pltpu.CompilerParams(vmem_limit_bytes=24 * 2**20),
        cost_estimate=pl.CostEstimate(flops=40_000_000, bytes_accessed=12 * 4 * planes[0].size, transcendentals=0),
        name="finish",
    )(*planes, *edge_stats, *inner_stats)
    shape = (depth, width, 4, lanes)
    return score.reshape(shape), end.reshape(shape)


def from_all(x):
    return [x] + [shift(x, "lon", by) for by in (1, -1, 2)]


def local(initial_heat, diffusivity_ratio, forcing_term):
    depth, width, _, lanes = initial_heat.shape
    plane = (depth, width)
    views = [a.reshape(depth, width, 4, 1, lanes) for a in (initial_heat, diffusivity_ratio, forcing_term)]
    u = [None] * 4
    (u[3],) = take(views[0], [plane], [plane_of(3, depth, 8)])
    up = shift(u[3], "lev", 1)
    u[0], south, north, east, west = take(
        views[0],
        [plane, (4, width), (4, width), (4, depth), (4, depth)],
        [
            plane_of(0, depth, 8),
            edge_of(lambda w, z: w.at[depth - 1, :, z]),
            edge_of(lambda w, z: w.at[0, :, z]),
            edge_of(lambda w, z: w.at[:, width - 1, z]),
            edge_of(lambda w, z: w.at[:, 0, z]),
        ],
    )
    whole = exchange(south, north, east, west)
    down = shift(u[0], "lev", -1)
    u[1], u[2] = take(views[0], [plane] * 2, [plane_of(z, depth, 8) for z in (1, 2)])
    d = take(views[1], [plane] * 4, [plane_of(z, depth, 8) for z in range(4)])
    f = take(views[2], [plane] * 4, [plane_of(z, depth, 8) for z in range(4)])
    where = [(whole, z) for z in range(4)]
    for step in range(STEPS):
        last = step == STEPS - 1
        first, second = (0, 3) if step % 2 == 0 else (3, 0)
        v = [None] * 4
        faces, stats = {}, {}
        carried = ()
        most = (first, 1, 2) if first == 0 else (3, 2, 1)
        for slot, zs in (("a", most), ("b", (second,))):
            made, rest = grow(zs, u, up, down, d, f, where, last, carried)
            for z, plane_made in zip(zs, made):
                v[z] = plane_made
            if last:
                stats[slot] = from_all(rest[0])
                continue
            if slot == "a":
                carried = rest
            else:
                sides = exchange(*rest)
            z = zs[0]
            faces[z] = shift(v[z], "lev", -1 if z == 0 else 1)
        if not last:
            order = most + (second,)
            where = [(sides, order.index(z)) for z in range(4)]
            up, down = faces[3], faces[0]
        u = v
    return finish(u, stats["b"], stats["a"])


def solution(mesh):
    placed = P("lat", "lon", "lev", None)

    return jax.shard_map(
        local,
        mesh=mesh,
        in_specs=(placed,) * 3,
        out_specs=(placed, placed),
        check_vma=False,
    )
```

```python
import jax
import jax.numpy as jnp
from jax import lax
from jax.experimental import pallas as pl
from jax.experimental.pallas import tpu as pltpu
from jax.sharding import PartitionSpec as P


STEPS = 4
ROWS = 8
BAND = 4
CUT = 16


def shift(x, axis, by):
    size = lax.axis_size(axis)
    return lax.ppermute(x, axis, [(i, (i + by) % size) for i in range(size)])


def take_body(parts, whole, low_row, *refs):
    outs, sems = refs[:-1], refs[-1]
    copies = []
    for n, (out, part) in enumerate(zip(outs, parts)):
        copies += [
            pltpu.make_async_copy(source(whole, low_row[0]), target(out), sems.at[n, k])
            for k, (source, target) in enumerate(part)
        ]
    for copy in copies:
        copy.start()
    for copy in copies:
        copy.wait()


def take(whole, low_row, shapes, parts, limit=10):
    lanes = whole.shape[-1]
    got = pl.pallas_call(
        lambda *refs: take_body(parts, *refs),
        in_specs=[pl.BlockSpec(memory_space=pltpu.HBM), pl.BlockSpec(memory_space=pltpu.SMEM)],
        out_specs=[pl.BlockSpec(memory_space=pltpu.VMEM)] * len(shapes),
        out_shape=[jax.ShapeDtypeStruct((*s, 1, lanes), whole.dtype) for s in shapes],
        scratch_shapes=[pltpu.SemaphoreType.DMA((len(parts), max(len(p) for p in parts)))],
        compiler_params=pltpu.CompilerParams(vmem_limit_bytes=limit * 2**20),
        cost_estimate=pl.CostEstimate(flops=20_000_000, bytes_accessed=2**22, transcendentals=0),
        name="take",
    )(whole, low_row)
    return [g.reshape(*s, lanes) for g, s in zip(got, shapes)]


def split_body(zs, whole, *outs):
    width = outs[0].shape[1]

    @pl.loop(0, ROWS)
    def _(r):
        for z, out in zip(zs, outs):
            out[r] = whole[r, pl.ds(z, width, stride=4), :]


def split(whole, zs):
    depth, wide, lanes = whole.shape
    width = wide // 4
    return pl.pallas_call(
        lambda *refs: split_body(zs, *refs),
        grid=(depth // ROWS,),
        in_specs=[pl.BlockSpec((ROWS, wide, lanes), lambda i: (i, 0, 0))],
        out_specs=[pl.BlockSpec((ROWS, width, lanes), lambda i: (i, 0, 0))] * len(zs),
        out_shape=[jax.ShapeDtypeStruct((depth, width, lanes), whole.dtype)] * len(zs),
        compiler_params=pltpu.CompilerParams(vmem_limit_bytes=9 * 2**20),
        cost_estimate=pl.CostEstimate(flops=20_000_000, bytes_accessed=2**24, transcendentals=0),
        name="split",
    )(whole)


def face_of(z, rows):
    cuts = list(range(0, rows, 4)) + [rows]

    def piece(start, size):
        return (lambda w, low: w.at[pl.ds(low + start, size), :, z], lambda o: o.at[pl.ds(start, size)])

    return [piece(start, stop - start) for start, stop in zip(cuts, cuts[1:])]


def edge_of(pick):
    return [(lambda w, low, z=z: pick(w, z), lambda o, z=z: o.at[z]) for z in range(4)]


def halo_row(pieces, edge, low_row, depth, g):
    at = g - low_row
    row, start = None, 0
    for piece in pieces:
        rows = piece.shape[0]
        here = piece[jnp.clip(at - start, 0, rows - 1)]
        row = here if row is None else jnp.where(at < start, row, here)
        start += rows
    return jnp.where(g == (depth - 1) * (1 - low_row), edge, row)


def grow_body(plan, last, *refs):
    zs, n_in, base, depth = plan["zs"], plan["n_in"], plan["base"], plan["depth"]
    ins, outs = refs[:n_in], refs[n_in:]
    i = pl.program_id(0)
    n = pl.num_programs(0)
    width = outs[0].shape[1]
    place = lax.broadcasted_iota(jnp.int32, outs[0].shape[1:], 0)
    for j, z in enumerate(zs):
        c, before, after, d, f, south, north, west, east = (ins[a] for a in plan[z])
        low, high = ([ins[a] for a in plan[side, z]] for side in ("low", "high"))
        rest = outs[len(zs) :]

        @pl.loop(0, BAND, unroll=4 if last else 2)
        def _(r, c=c, low=low, high=high, before=before, after=after, d=d, f=f, south=south, north=north, west=west, east=east, j=j):
            x = c[r]
            edge_low = jnp.where(i == 0, south[0], before[0])
            edge_high = jnp.where(i == n - 1, north[0], after[0])
            lat_low = jnp.where(r == 0, edge_low, c[jnp.maximum(r - 1, 0)])
            lat_high = jnp.where(r == BAND - 1, edge_high, c[jnp.minimum(r + 1, BAND - 1)])
            left = jnp.where(place == 0, west[0, pl.ds(i * BAND + r, 1), :], pltpu.roll(x, 1, 0))
            right = jnp.where(place == width - 1, east[0, pl.ds(i * BAND + r, 1), :], pltpu.roll(x, width - 1, 0))
            below, above = (
                halo_row(h[:1], h[1][0], ins[0][0], depth, i * BAND + r) if len(h) == 2 else h[0][r] for h in (low, high)
            )
            spread = lat_low + lat_high + left + right + below + above - 6.0 * x
            y = x + d[r] * spread + f[r]
            outs[j][r] = y
            if last:
                total = jnp.sum(y, axis=0, keepdims=True)
                away = y - total * (1.0 / width)
                rest[0][2 * j, pl.ds(i * BAND + r, 1), :] = total
                rest[0][2 * j + 1, pl.ds(i * BAND + r, 1), :] = jnp.sum(away * away, axis=0, keepdims=True)
            else:
                rest[2][base + j, pl.ds(i * BAND + r, 1), :] = y[width - 1 :, :]
                rest[3][base + j, pl.ds(i * BAND + r, 1), :] = y[:1, :]

        if not last:

            @pl.when(i == 0)
            def _(j=j):
                rest[1][base + j] = outs[j][0]

            @pl.when(i == n - 1)
            def _(j=j):
                rest[0][base + j] = outs[j][BAND - 1]

    if plan["carried"]:
        held = [ins[a] for a in plan["carried"]]

        @pl.when(i == 0)
        def _():
            for k in range(4):
                rest[k][:base] = held[k][...]


def grow(zs, low_row, u, low, high, d, f, where, last, carried=()):
    depth, width, lanes = u[0].shape
    block = pl.BlockSpec((BAND, width, lanes), lambda i: (i, 0, 0))
    row_before = pl.BlockSpec((1, width, lanes), lambda i: (jnp.maximum(i * BAND - 1, 0), 0, 0))
    row_after = pl.BlockSpec((1, width, lanes), lambda i: (jnp.minimum(i * BAND + BAND, depth - 1), 0, 0))
    whole_face = pl.BlockSpec((depth - 1, width, lanes), lambda i: (0, 0, 0))
    whole_row = pl.BlockSpec((1, width, lanes), lambda i: (0, 0, 0))
    arrays, specs, seen = [low_row], [pl.BlockSpec(memory_space=pltpu.SMEM)], {}

    def use(key, array, spec):
        if key not in seen:
            seen[key] = len(arrays)
            arrays.append(array)
            specs.append(spec)
        return seen[key]

    plan = {"zs": zs, "depth": depth}
    for z in zs:
        sides, k = where[z]
        lat_edge = pl.BlockSpec((1, width, lanes), lambda i, k=k: (k, 0, 0))
        lon_edge = pl.BlockSpec((1, depth, lanes), lambda i, k=k: (k, 0, 0))
        plan[z] = [
            use(("u", z), u[z], block),
            use(("before", z), u[z], row_before),
            use(("after", z), u[z], row_after),
            use(("d", z), d[z], block),
            use(("f", z), f[z], block),
            use(("s", z), sides[0], lat_edge),
            use(("n", z), sides[1], lat_edge),
            use(("w", z), sides[2], lon_edge),
            use(("e", z), sides[3], lon_edge),
        ]
    for z in zs:
        for side, outer, halo, other in (("low", 0, low, z - 1), ("high", 3, high, z + 1)):
            if z == outer:
                plan[side, z] = [use((side, 0), halo[0], whole_face), use((side, 1), halo[1], whole_row)]
            else:
                plan[side, z] = [use(("u", other), u[other], block)]
    m = len(zs)
    base = carried[0].shape[0] if carried else 0
    lat_all = pl.BlockSpec((base, width, lanes), lambda i: (0, 0, 0))
    lon_all = pl.BlockSpec((base, depth, lanes), lambda i: (0, 0, 0))
    plan["carried"] = [
        use(("carried", k), a, spec) for k, (a, spec) in enumerate(zip(carried, (lat_all, lat_all, lon_all, lon_all)))
    ]
    plan["base"], plan["n_in"] = base, len(arrays)
    shapes, outs = [u[0].shape] * m, [block] * m
    if last:
        shapes += [(2 * m, depth, lanes)]
        outs += [pl.BlockSpec((2 * m, depth, lanes), lambda i: (0, 0, 0))]
    else:
        t = base + m
        shapes += [(t, width, lanes)] * 2 + [(t, depth, lanes)] * 2
        outs += [pl.BlockSpec((t, width, lanes), lambda i: (0, 0, 0))] * 2
        outs += [pl.BlockSpec((t, depth, lanes), lambda i: (0, 0, 0))] * 2
    got = pl.pallas_call(
        lambda *refs: grow_body(plan, last, *refs),
        grid=(depth // BAND,),
        in_specs=specs,
        out_specs=outs,
        out_shape=[jax.ShapeDtypeStruct(s, u[0].dtype) for s in shapes],
        compiler_params=pltpu.CompilerParams(vmem_limit_bytes=(8 if m == 1 else 13) * 2**20),
        cost_estimate=pl.CostEstimate(flops=10_000_000 * m, bytes_accessed=2**22 * m, transcendentals=0),
        name="grow",
    )(*arrays)
    return got[:m], got[m:]


def exchange(south, north, east, west):
    return (
        shift(south, "lat", 1),
        shift(north, "lat", -1),
        shift(east, "lon", 1),
        shift(west, "lon", -1),
    )


def scale_of(count, width, own, others, k):
    sums = [s[2 * k] for s in (own, *others)]
    powers = [s[2 * k + 1] for s in (own, *others)]
    mean = (sums[0] + sums[1] + sums[2] + sums[3]) * (1.0 / count)
    power = powers[0] + powers[1] + powers[2] + powers[3]
    for s in sums:
        gap = s * (1.0 / width) - mean
        power = power + width * (gap * gap)
    return mean, lax.rsqrt(power * (1.0 / count) + 0.0001)


def finish_body(count, zs, *refs):
    m = len(zs)
    planes, stats, (score, end) = refs[:m], refs[m:-2], refs[-2:]
    width = planes[0].shape[1]
    for k, z in enumerate(zs):
        mean, scale = scale_of(count, width, stats[0], stats[1:], k)
        for r in range(ROWS):
            y = planes[k][r]
            end[r, pl.ds(z, width, stride=4), :] = y
            score[r, pl.ds(z, width, stride=4), :] = (y - mean[r : r + 1, :]) * scale[r : r + 1, :]


def finish(zs, planes, stats):
    depth, width, lanes = planes[0].shape
    m = len(zs)
    block = pl.BlockSpec((ROWS, width, lanes), lambda i: (i, 0, 0))
    wide = pl.BlockSpec((ROWS, 4 * width, lanes), lambda i: (i, 0, 0))
    stat = pl.BlockSpec((2 * m, ROWS, lanes), lambda i: (0, i, 0))
    count = width * lax.axis_size("lon")
    full = jax.ShapeDtypeStruct((depth, 4 * width, lanes), planes[0].dtype)
    return pl.pallas_call(
        lambda *refs: finish_body(count, zs, *refs),
        grid=(depth // ROWS,),
        in_specs=[block] * m + [stat] * 4,
        out_specs=[wide] * 2,
        out_shape=[full] * 2,
        compiler_params=pltpu.CompilerParams(vmem_limit_bytes=24 * 2**20),
        cost_estimate=pl.CostEstimate(flops=30_000_000, bytes_accessed=2**24, transcendentals=0),
        name="finish",
    )(*planes, *stats)


def put_body(start, _, source, out, sems):
    copies = [
        pltpu.make_async_copy(
            source.at[pl.ds(k * ROWS, ROWS)], out.at[pl.ds(start + k * ROWS, ROWS), :, 0], sems.at[k]
        )
        for k in range(source.shape[0] // ROWS)
    ]
    for copy in copies:
        copy.start()
    for copy in copies:
        copy.wait()


def put(view, rows, start):
    depth, width, lanes = rows.shape
    return pl.pallas_call(
        lambda *refs: put_body(start, *refs),
        in_specs=[pl.BlockSpec(memory_space=pltpu.HBM), pl.BlockSpec(memory_space=pltpu.VMEM)],
        out_specs=pl.BlockSpec(memory_space=pltpu.HBM),
        out_shape=jax.ShapeDtypeStruct(view.shape, view.dtype),
        scratch_shapes=[pltpu.SemaphoreType.DMA((depth // ROWS,))],
        input_output_aliases={0: 0},
        compiler_params=pltpu.CompilerParams(vmem_limit_bytes=2**20),
        cost_estimate=pl.CostEstimate(flops=5_000_000, bytes_accessed=2**21, transcendentals=0),
        name="put",
    )(view, rows.reshape(depth, width, 1, lanes))


def put_scaled_body(count, start, _, plane, own, s1, s2, s3, out, held, sems):
    depth, width, _ = plane.shape
    mean, scale = scale_of(count, width, own, (s1, s2, s3), 0)
    copies = []
    for k in range(depth // ROWS):
        for r in range(k * ROWS, (k + 1) * ROWS):
            held[r, :, 0, :] = (plane[r] - mean[r : r + 1, :]) * scale[r : r + 1, :]
        copies.append(
            pltpu.make_async_copy(
                held.at[pl.ds(k * ROWS, ROWS)], out.at[pl.ds(start + k * ROWS, ROWS), :, 0], sems.at[k]
            )
        )
        copies[-1].start()
    for copy in copies:
        copy.wait()


def put_scaled(view, rows, stats, start):
    depth, width, lanes = rows.shape
    count = width * lax.axis_size("lon")
    return pl.pallas_call(
        lambda *refs: put_scaled_body(count, start, *refs),
        in_specs=[pl.BlockSpec(memory_space=pltpu.HBM)] + [pl.BlockSpec(memory_space=pltpu.VMEM)] * 5,
        out_specs=pl.BlockSpec(memory_space=pltpu.HBM),
        out_shape=jax.ShapeDtypeStruct(view.shape, view.dtype),
        scratch_shapes=[
            pltpu.VMEM((depth, width, 1, lanes), rows.dtype),
            pltpu.SemaphoreType.DMA((depth // ROWS,)),
        ],
        input_output_aliases={0: 0},
        compiler_params=pltpu.CompilerParams(vmem_limit_bytes=4 * 2**20),
        cost_estimate=pl.CostEstimate(flops=5_000_000, bytes_accessed=2**21, transcendentals=0),
        name="put_scaled",
    )(view, rows, *stats)


def grow_last_body(start, k, low_row, c, high, d, f, south, north, west, east, edge, *refs):
    pieces, (out, stat) = refs[:-2], refs[-2:]
    depth, width, _ = c.shape
    rows = out.shape[0]
    place = lax.broadcasted_iota(jnp.int32, c.shape[1:], 0)

    @pl.loop(0, rows, unroll=2)
    def _(i):
        r = start + i
        x = c[r]
        lat_low = jnp.where(r == 0, south[k], c[jnp.maximum(r - 1, 0)])
        lat_high = jnp.where(r == depth - 1, north[k], c[jnp.minimum(r + 1, depth - 1)])
        left = jnp.where(place == 0, west[k, pl.ds(r, 1), :], pltpu.roll(x, 1, 0))
        right = jnp.where(place == width - 1, east[k, pl.ds(r, 1), :], pltpu.roll(x, width - 1, 0))
        below = halo_row(pieces, edge[0], low_row[0], depth, r)
        spread = lat_low + lat_high + left + right + below + high[r] - 6.0 * x
        y = x + d[r] * spread + f[r]
        out[i] = y
        total = jnp.sum(y, axis=0, keepdims=True)
        away = y - total * (1.0 / width)
        stat[0, pl.ds(i, 1), :] = total
        stat[1, pl.ds(i, 1), :] = jnp.sum(away * away, axis=0, keepdims=True)


def grow_last(start, rows, low_row, u, pieces, edge, d, f, where):
    sides, k = where
    _, width, lanes = u[0].shape
    vmem = pl.BlockSpec(memory_space=pltpu.VMEM)
    return pl.pallas_call(
        lambda *refs: grow_last_body(start, k, *refs),
        in_specs=[pl.BlockSpec(memory_space=pltpu.SMEM)] + [vmem] * (9 + len(pieces)),
        out_specs=[vmem] * 2,
        out_shape=[
            jax.ShapeDtypeStruct((rows, width, lanes), u[0].dtype),
            jax.ShapeDtypeStruct((2, rows, lanes), u[0].dtype),
        ],
        compiler_params=pltpu.CompilerParams(vmem_limit_bytes=2**20),
        cost_estimate=pl.CostEstimate(flops=10_000_000, bytes_accessed=2**22, transcendentals=0),
        name="grow_last",
    )(low_row, u[0], u[1], d, f, *sides, edge, *pieces)


def from_all(x):
    return [x] + [shift(x, "lon", by) for by in (1, -1, 2)]


def local_call(body, shapes, low_row, *arrays):
    vmem = pl.BlockSpec(memory_space=pltpu.VMEM)
    return pl.pallas_call(
        body,
        in_specs=[pl.BlockSpec(memory_space=pltpu.SMEM)] + [vmem] * len(arrays),
        out_specs=[vmem] * len(shapes),
        out_shape=[jax.ShapeDtypeStruct(s, arrays[0].dtype) for s in shapes],
        compiler_params=pltpu.CompilerParams(vmem_limit_bytes=2**20),
        cost_estimate=pl.CostEstimate(flops=2_000_000, bytes_accessed=2**21, transcendentals=0),
    )(low_row, *arrays)


def pick(sides, places, low_row):
    def body(low, south, north, *outs):
        for place, out in zip(places, outs):
            out[0] = jnp.where(low[0] == 1, south[place], north[place])

    return local_call(body, [(1, *sides[0].shape[1:])] * len(places), low_row, *sides[:2])


def cut(plane, start, rows, low_row):
    def body(low, whole, out):
        @pl.loop(0, rows)
        def _(r):
            out[r] = whole[low[0] + start + r]

    return local_call(body, [(rows, *plane.shape[1:])], low_row, plane)[0]


def relay(row, by):
    lat, lev = lax.axis_size("lat"), lax.axis_size("lev")
    pairs = []
    for a in range(lat):
        for b in range(lev):
            to = (a + (1 if a % 2 else -1)) % lat, (b + by) % lev
            pairs.append((a * lev + b, to[0] * lev + to[1]))
    return lax.ppermute(row, ("lat", "lev"), pairs)


def local(initial_heat, diffusivity_ratio, forcing_term):
    depth, width, _, lanes = initial_heat.shape
    face = (depth - 1, width)
    view = initial_heat.reshape(depth, width, 4, 1, lanes)
    raw, d, f = (a.reshape(depth, 4 * width, lanes) for a in (initial_heat, diffusivity_ratio, forcing_term))
    low_start = 1 - lax.axis_index("lat") % 2
    low_row = jnp.full((1,), low_start, jnp.int32)
    (send,) = take(view, low_row, [face], [face_of(3, depth - 1)], 50)
    up = shift(send, "lev", 1)
    send, *rest = take(
        view,
        low_row,
        [face, (4, width), (4, width), (4, depth), (4, depth)],
        [
            face_of(0, depth - 1),
            edge_of(lambda w, z: w.at[depth - 1, :, z]),
            edge_of(lambda w, z: w.at[0, :, z]),
            edge_of(lambda w, z: w.at[:, width - 1, z]),
            edge_of(lambda w, z: w.at[:, 0, z]),
        ],
        50,
    )
    sides = exchange(*rest)
    down = shift(send, "lev", -1)
    u, d, f = (split(a, (0, 1, 2, 3)) for a in (raw, d, f))
    order = (0, 1, 2, 3)
    for step in range(STEPS):
        where = [(sides, order.index(z)) for z in range(4)]
        rows = pick(sides, (order.index(3), order.index(0)), low_row)
        low, high = (up, relay(rows[0], 1)), (down, relay(rows[1], -1))
        if step == STEPS - 1:
            break
        first, second = (0, 3) if step % 2 == 0 else (3, 0)
        most = (first, 1, 2) if first == 0 else (3, 2, 1)
        made, carried = grow(most, low_row, u, low, high, d, f, where, False)
        early = shift(cut(made[0], 0, depth - 1, low_row), "lev", -1 if first == 0 else 1)
        (v,), rest = grow((second,), low_row, u, low, high, d, f, where, False, carried)
        sides = exchange(*rest)
        if step < STEPS - 2:
            late = shift(cut(v, 0, depth - 1, low_row), "lev", -1 if second == 0 else 1)
        else:
            late = [shift(cut(v, 0, CUT, low_row), "lev", 1)]
            late.append(shift(cut(v, CUT, depth - 1 - CUT, low_row), "lev", 1))
        order = most + (second,)
        made = dict(zip(order, [*made, v]))
        u = [made[z] for z in range(4)]
        up, down = (late, early) if first == 0 else (early, late)
    made, (stat,) = grow((3, 2, 1), low_row, u, low, high, d, f, where, True)
    stats = from_all(stat)
    filled = finish((3, 2, 1), made, stats)
    score, end = (x.reshape(depth, width, 4, 1, lanes) for x in filled)
    pieces, edge = low
    for name, start, stop in (("b", 0, CUT), ("c", CUT, depth)):
        near = pieces[:1] if name == "b" else pieces
        rows, stat = grow_last(start, stop - start, low_row, u, near, edge, d[0], f[0], where[0])
        stats = from_all(stat)
        end = put(end, rows, start)
        score = put_scaled(score, rows, stats, start)
    return score.reshape(initial_heat.shape), end.reshape(initial_heat.shape)


def solution(mesh):
    placed = P("lat", "lon", "lev", None)

    return jax.shard_map(
        local,
        mesh=mesh,
        in_specs=(placed,) * 3,
        out_specs=(placed, placed),
        check_vma=False,
    )
```

```python
import jax
import jax.numpy as jnp
from jax import lax
from jax.experimental import pallas as pl
from jax.experimental.pallas import tpu as pltpu
from jax.sharding import PartitionSpec as P


STEPS = 4
ROWS = 8
BAND = 4
CUT = 24


def shift(x, axis, by):
    size = lax.axis_size(axis)
    return lax.ppermute(x, axis, [(i, (i + by) % size) for i in range(size)])


def take_body(parts, whole, low_row, *refs):
    outs, sems = refs[:-1], refs[-1]
    copies = []
    for n, (out, part) in enumerate(zip(outs, parts)):
        copies += [
            pltpu.make_async_copy(source(whole, low_row[0]), target(out), sems.at[n, k])
            for k, (source, target) in enumerate(part)
        ]
    for copy in copies:
        copy.start()
    for copy in copies:
        copy.wait()


def take(whole, low_row, shapes, parts, limit=10):
    lanes = whole.shape[-1]
    got = pl.pallas_call(
        lambda *refs: take_body(parts, *refs),
        in_specs=[pl.BlockSpec(memory_space=pltpu.HBM), pl.BlockSpec(memory_space=pltpu.SMEM)],
        out_specs=[pl.BlockSpec(memory_space=pltpu.VMEM)] * len(shapes),
        out_shape=[jax.ShapeDtypeStruct((*s, 1, lanes), whole.dtype) for s in shapes],
        scratch_shapes=[pltpu.SemaphoreType.DMA((len(parts), max(len(p) for p in parts)))],
        compiler_params=pltpu.CompilerParams(vmem_limit_bytes=limit * 2**20),
        cost_estimate=pl.CostEstimate(flops=20_000_000, bytes_accessed=2**22, transcendentals=0),
        name="take",
    )(whole, low_row)
    return [g.reshape(*s, lanes) for g, s in zip(got, shapes)]


def split_body(zs, whole, *outs):
    width = outs[0].shape[1]

    @pl.loop(0, ROWS)
    def _(r):
        for z, out in zip(zs, outs):
            out[r] = whole[r, pl.ds(z, width, stride=4), :]


def split(whole, zs):
    depth, wide, lanes = whole.shape
    width = wide // 4
    return pl.pallas_call(
        lambda *refs: split_body(zs, *refs),
        grid=(depth // ROWS,),
        in_specs=[pl.BlockSpec((ROWS, wide, lanes), lambda i: (i, 0, 0))],
        out_specs=[pl.BlockSpec((ROWS, width, lanes), lambda i: (i, 0, 0))] * len(zs),
        out_shape=[jax.ShapeDtypeStruct((depth, width, lanes), whole.dtype)] * len(zs),
        compiler_params=pltpu.CompilerParams(vmem_limit_bytes=9 * 2**20),
        cost_estimate=pl.CostEstimate(flops=20_000_000, bytes_accessed=2**24, transcendentals=0),
        name="split",
    )(whole)


def face_of(z, rows):
    cuts = list(range(0, rows, 4)) + [rows]

    def piece(start, size):
        return (lambda w, low: w.at[pl.ds(low + start, size), :, z], lambda o: o.at[pl.ds(start, size)])

    return [piece(start, stop - start) for start, stop in zip(cuts, cuts[1:])]


def edge_of(pick):
    return [(lambda w, low, z=z: pick(w, z), lambda o, z=z: o.at[z]) for z in range(4)]


def halo_row(pieces, edge, low_row, depth, g):
    at = g - low_row
    row, start = None, 0
    for piece in pieces:
        rows = piece.shape[0]
        here = piece[jnp.clip(at - start, 0, rows - 1)]
        row = here if row is None else jnp.where(at < start, row, here)
        start += rows
    return jnp.where(g == (depth - 1) * (1 - low_row), edge, row)


def grow_body(plan, last, *refs):
    zs, n_in, base, depth = plan["zs"], plan["n_in"], plan["base"], plan["depth"]
    ins, outs = refs[:n_in], refs[n_in:]
    i = pl.program_id(0)
    n = pl.num_programs(0)
    width = outs[0].shape[1]
    place = lax.broadcasted_iota(jnp.int32, outs[0].shape[1:], 0)
    for j, z in enumerate(zs):
        c, before, after, d, f, south, north, west, east = (ins[a] for a in plan[z])
        low, high = ([ins[a] for a in plan[side, z]] for side in ("low", "high"))
        rest = outs[len(zs) :]

        @pl.loop(0, BAND, unroll=4 if last else 2)
        def _(r, c=c, low=low, high=high, before=before, after=after, d=d, f=f, south=south, north=north, west=west, east=east, j=j):
            x = c[r]
            edge_low = jnp.where(i == 0, south[0], before[0])
            edge_high = jnp.where(i == n - 1, north[0], after[0])
            lat_low = jnp.where(r == 0, edge_low, c[jnp.maximum(r - 1, 0)])
            lat_high = jnp.where(r == BAND - 1, edge_high, c[jnp.minimum(r + 1, BAND - 1)])
            left = jnp.where(place == 0, west[0, pl.ds(i * BAND + r, 1), :], pltpu.roll(x, 1, 0))
            right = jnp.where(place == width - 1, east[0, pl.ds(i * BAND + r, 1), :], pltpu.roll(x, width - 1, 0))
            below, above = (
                halo_row(h[:1], h[1][0], ins[0][0], depth, i * BAND + r) if len(h) == 2 else h[0][r] for h in (low, high)
            )
            spread = lat_low + lat_high + left + right + below + above - 6.0 * x
            y = x + d[r] * spread + f[r]
            outs[j][r] = y
            if last:
                total = jnp.sum(y, axis=0, keepdims=True)
                away = y - total * (1.0 / width)
                rest[0][2 * j, pl.ds(i * BAND + r, 1), :] = total
                rest[0][2 * j + 1, pl.ds(i * BAND + r, 1), :] = jnp.sum(away * away, axis=0, keepdims=True)
            else:
                rest[2][base + j, pl.ds(i * BAND + r, 1), :] = y[width - 1 :, :]
                rest[3][base + j, pl.ds(i * BAND + r, 1), :] = y[:1, :]

        if not last:

            @pl.when(i == 0)
            def _(j=j):
                rest[1][base + j] = outs[j][0]

            @pl.when(i == n - 1)
            def _(j=j):
                rest[0][base + j] = outs[j][BAND - 1]

    if plan["carried"]:
        held = [ins[a] for a in plan["carried"]]

        @pl.when(i == 0)
        def _():
            for k in range(4):
                rest[k][:base] = held[k][...]


def grow(zs, low_row, u, low, high, d, f, where, last, carried=()):
    depth, width, lanes = u[0].shape
    block = pl.BlockSpec((BAND, width, lanes), lambda i: (i, 0, 0))
    row_before = pl.BlockSpec((1, width, lanes), lambda i: (jnp.maximum(i * BAND - 1, 0), 0, 0))
    row_after = pl.BlockSpec((1, width, lanes), lambda i: (jnp.minimum(i * BAND + BAND, depth - 1), 0, 0))
    whole_face = pl.BlockSpec((depth - 1, width, lanes), lambda i: (0, 0, 0))
    whole_row = pl.BlockSpec((1, width, lanes), lambda i: (0, 0, 0))
    arrays, specs, seen = [low_row], [pl.BlockSpec(memory_space=pltpu.SMEM)], {}

    def use(key, array, spec):
        if key not in seen:
            seen[key] = len(arrays)
            arrays.append(array)
            specs.append(spec)
        return seen[key]

    plan = {"zs": zs, "depth": depth}
    for z in zs:
        sides, k = where[z]
        lat_edge = pl.BlockSpec((1, width, lanes), lambda i, k=k: (k, 0, 0))
        lon_edge = pl.BlockSpec((1, depth, lanes), lambda i, k=k: (k, 0, 0))
        plan[z] = [
            use(("u", z), u[z], block),
            use(("before", z), u[z], row_before),
            use(("after", z), u[z], row_after),
            use(("d", z), d[z], block),
            use(("f", z), f[z], block),
            use(("s", z), sides[0], lat_edge),
            use(("n", z), sides[1], lat_edge),
            use(("w", z), sides[2], lon_edge),
            use(("e", z), sides[3], lon_edge),
        ]
    for z in zs:
        for side, outer, halo, other in (("low", 0, low, z - 1), ("high", 3, high, z + 1)):
            if z == outer:
                plan[side, z] = [use((side, 0), halo[0], whole_face), use((side, 1), halo[1], whole_row)]
            else:
                plan[side, z] = [use(("u", other), u[other], block)]
    m = len(zs)
    base = carried[0].shape[0] if carried else 0
    lat_all = pl.BlockSpec((base, width, lanes), lambda i: (0, 0, 0))
    lon_all = pl.BlockSpec((base, depth, lanes), lambda i: (0, 0, 0))
    plan["carried"] = [
        use(("carried", k), a, spec) for k, (a, spec) in enumerate(zip(carried, (lat_all, lat_all, lon_all, lon_all)))
    ]
    plan["base"], plan["n_in"] = base, len(arrays)
    shapes, outs = [u[0].shape] * m, [block] * m
    if last:
        shapes += [(2 * m, depth, lanes)]
        outs += [pl.BlockSpec((2 * m, depth, lanes), lambda i: (0, 0, 0))]
    else:
        t = base + m
        shapes += [(t, width, lanes)] * 2 + [(t, depth, lanes)] * 2
        outs += [pl.BlockSpec((t, width, lanes), lambda i: (0, 0, 0))] * 2
        outs += [pl.BlockSpec((t, depth, lanes), lambda i: (0, 0, 0))] * 2
    got = pl.pallas_call(
        lambda *refs: grow_body(plan, last, *refs),
        grid=(depth // BAND,),
        in_specs=specs,
        out_specs=outs,
        out_shape=[jax.ShapeDtypeStruct(s, u[0].dtype) for s in shapes],
        compiler_params=pltpu.CompilerParams(vmem_limit_bytes=(8 if m == 1 else 13) * 2**20),
        cost_estimate=pl.CostEstimate(flops=10_000_000 * m, bytes_accessed=2**22 * m, transcendentals=0),
        name="grow",
    )(*arrays)
    return got[:m], got[m:]


def exchange(south, north, east, west):
    return (
        shift(south, "lat", 1),
        shift(north, "lat", -1),
        shift(east, "lon", 1),
        shift(west, "lon", -1),
    )


def scale_of(count, width, own, others, k):
    sums = [s[2 * k] for s in (own, *others)]
    powers = [s[2 * k + 1] for s in (own, *others)]
    mean = (sums[0] + sums[1] + sums[2] + sums[3]) * (1.0 / count)
    power = powers[0] + powers[1] + powers[2] + powers[3]
    for s in sums:
        gap = s * (1.0 / width) - mean
        power = power + width * (gap * gap)
    return mean, lax.rsqrt(power * (1.0 / count) + 0.0001)


def finish_body(count, zs, *refs):
    m = len(zs)
    planes, stats, (score, end) = refs[:m], refs[m:-2], refs[-2:]
    width = planes[0].shape[1]
    for k, z in enumerate(zs):
        mean, scale = scale_of(count, width, stats[0], stats[1:], k)
        for r in range(ROWS):
            y = planes[k][r]
            end[r, pl.ds(z, width, stride=4), :] = y
            score[r, pl.ds(z, width, stride=4), :] = (y - mean[r : r + 1, :]) * scale[r : r + 1, :]


def finish(zs, planes, stats):
    depth, width, lanes = planes[0].shape
    m = len(zs)
    block = pl.BlockSpec((ROWS, width, lanes), lambda i: (i, 0, 0))
    wide = pl.BlockSpec((ROWS, 4 * width, lanes), lambda i: (i, 0, 0))
    stat = pl.BlockSpec((2 * m, ROWS, lanes), lambda i: (0, i, 0))
    count = width * lax.axis_size("lon")
    full = jax.ShapeDtypeStruct((depth, 4 * width, lanes), planes[0].dtype)
    return pl.pallas_call(
        lambda *refs: finish_body(count, zs, *refs),
        grid=(depth // ROWS,),
        in_specs=[block] * m + [stat] * 4,
        out_specs=[wide] * 2,
        out_shape=[full] * 2,
        compiler_params=pltpu.CompilerParams(vmem_limit_bytes=24 * 2**20),
        cost_estimate=pl.CostEstimate(flops=30_000_000, bytes_accessed=2**24, transcendentals=0),
        name="finish",
    )(*planes, *stats)


def put_body(start, _, source, out, sems):
    copies = [
        pltpu.make_async_copy(
            source.at[pl.ds(k * BAND, BAND)], out.at[pl.ds(start + k * BAND, BAND), :, 0], sems.at[k]
        )
        for k in range(source.shape[0] // BAND)
    ]
    for copy in copies:
        copy.start()
    for copy in copies:
        copy.wait()


def put(view, rows, start):
    depth, width, lanes = rows.shape
    return pl.pallas_call(
        lambda *refs: put_body(start, *refs),
        in_specs=[pl.BlockSpec(memory_space=pltpu.HBM), pl.BlockSpec(memory_space=pltpu.VMEM)],
        out_specs=pl.BlockSpec(memory_space=pltpu.HBM),
        out_shape=jax.ShapeDtypeStruct(view.shape, view.dtype),
        scratch_shapes=[pltpu.SemaphoreType.DMA((depth // BAND,))],
        input_output_aliases={0: 0},
        compiler_params=pltpu.CompilerParams(vmem_limit_bytes=2**20),
        cost_estimate=pl.CostEstimate(flops=5_000_000, bytes_accessed=2**21, transcendentals=0),
        name="put",
    )(view, rows.reshape(depth, width, 1, lanes))


def put_scaled_body(count, start, _, plane, own, s1, s2, s3, out, held, sems):
    depth, width, _ = plane.shape
    mean, scale = scale_of(count, width, own, (s1, s2, s3), 0)
    copies = []
    for k in range(depth // BAND):
        for r in range(k * BAND, (k + 1) * BAND):
            held[r, :, 0, :] = (plane[r] - mean[r : r + 1, :]) * scale[r : r + 1, :]
        copies.append(
            pltpu.make_async_copy(
                held.at[pl.ds(k * BAND, BAND)], out.at[pl.ds(start + k * BAND, BAND), :, 0], sems.at[k]
            )
        )
        copies[-1].start()
    for copy in copies:
        copy.wait()


def put_scaled(view, rows, stats, start):
    depth, width, lanes = rows.shape
    count = width * lax.axis_size("lon")
    return pl.pallas_call(
        lambda *refs: put_scaled_body(count, start, *refs),
        in_specs=[pl.BlockSpec(memory_space=pltpu.HBM)] + [pl.BlockSpec(memory_space=pltpu.VMEM)] * 5,
        out_specs=pl.BlockSpec(memory_space=pltpu.HBM),
        out_shape=jax.ShapeDtypeStruct(view.shape, view.dtype),
        scratch_shapes=[
            pltpu.VMEM((depth, width, 1, lanes), rows.dtype),
            pltpu.SemaphoreType.DMA((depth // BAND,)),
        ],
        input_output_aliases={0: 0},
        compiler_params=pltpu.CompilerParams(vmem_limit_bytes=4 * 2**20),
        cost_estimate=pl.CostEstimate(flops=5_000_000, bytes_accessed=2**21, transcendentals=0),
        name="put_scaled",
    )(view, rows, *stats)


def grow_last_body(start, k, low_row, c, high, d, f, south, north, west, east, edge, *refs):
    pieces, (out, stat) = refs[:-2], refs[-2:]
    depth, width, _ = c.shape
    rows = out.shape[0]
    place = lax.broadcasted_iota(jnp.int32, c.shape[1:], 0)

    @pl.loop(0, rows, unroll=2)
    def _(i):
        r = start + i
        x = c[r]
        lat_low = jnp.where(r == 0, south[k], c[jnp.maximum(r - 1, 0)])
        lat_high = jnp.where(r == depth - 1, north[k], c[jnp.minimum(r + 1, depth - 1)])
        left = jnp.where(place == 0, west[k, pl.ds(r, 1), :], pltpu.roll(x, 1, 0))
        right = jnp.where(place == width - 1, east[k, pl.ds(r, 1), :], pltpu.roll(x, width - 1, 0))
        below = halo_row(pieces, edge[0], low_row[0], depth, r)
        spread = lat_low + lat_high + left + right + below + high[r] - 6.0 * x
        y = x + d[r] * spread + f[r]
        out[i] = y
        total = jnp.sum(y, axis=0, keepdims=True)
        away = y - total * (1.0 / width)
        stat[0, pl.ds(i, 1), :] = total
        stat[1, pl.ds(i, 1), :] = jnp.sum(away * away, axis=0, keepdims=True)


def grow_last(start, rows, low_row, u, pieces, edge, d, f, where):
    sides, k = where
    _, width, lanes = u[0].shape
    vmem = pl.BlockSpec(memory_space=pltpu.VMEM)
    return pl.pallas_call(
        lambda *refs: grow_last_body(start, k, *refs),
        in_specs=[pl.BlockSpec(memory_space=pltpu.SMEM)] + [vmem] * (9 + len(pieces)),
        out_specs=[vmem] * 2,
        out_shape=[
            jax.ShapeDtypeStruct((rows, width, lanes), u[0].dtype),
            jax.ShapeDtypeStruct((2, rows, lanes), u[0].dtype),
        ],
        compiler_params=pltpu.CompilerParams(vmem_limit_bytes=2**20),
        cost_estimate=pl.CostEstimate(flops=10_000_000, bytes_accessed=2**22, transcendentals=0),
        name="grow_last",
    )(low_row, u[0], u[1], d, f, *sides, edge, *pieces)


def from_all(x):
    return [x] + [shift(x, "lon", by) for by in (1, -1, 2)]


def local_call(body, shapes, low_row, *arrays):
    vmem = pl.BlockSpec(memory_space=pltpu.VMEM)
    return pl.pallas_call(
        body,
        in_specs=[pl.BlockSpec(memory_space=pltpu.SMEM)] + [vmem] * len(arrays),
        out_specs=[vmem] * len(shapes),
        out_shape=[jax.ShapeDtypeStruct(s, arrays[0].dtype) for s in shapes],
        compiler_params=pltpu.CompilerParams(vmem_limit_bytes=2**20),
        cost_estimate=pl.CostEstimate(flops=2_000_000, bytes_accessed=2**21, transcendentals=0),
    )(low_row, *arrays)


def pick(sides, places, low_row):
    def body(low, south, north, *outs):
        for place, out in zip(places, outs):
            out[0] = jnp.where(low[0] == 1, south[place], north[place])

    return local_call(body, [(1, *sides[0].shape[1:])] * len(places), low_row, *sides[:2])


def cut(plane, start, rows, low_row):
    def body(low, whole, out):
        @pl.loop(0, rows)
        def _(r):
            out[r] = whole[low[0] + start + r]

    return local_call(body, [(rows, *plane.shape[1:])], low_row, plane)[0]


def relay(row, by):
    lat, lev = lax.axis_size("lat"), lax.axis_size("lev")
    pairs = []
    for a in range(lat):
        for b in range(lev):
            to = (a + (1 if a % 2 else -1)) % lat, (b + by) % lev
            pairs.append((a * lev + b, to[0] * lev + to[1]))
    return lax.ppermute(row, ("lat", "lev"), pairs)


def local(initial_heat, diffusivity_ratio, forcing_term):
    depth, width, _, lanes = initial_heat.shape
    face = (depth - 1, width)
    view = initial_heat.reshape(depth, width, 4, 1, lanes)
    raw, d, f = (a.reshape(depth, 4 * width, lanes) for a in (initial_heat, diffusivity_ratio, forcing_term))
    low_start = 1 - lax.axis_index("lat") % 2
    low_row = jnp.full((1,), low_start, jnp.int32)
    (send,) = take(view, low_row, [face], [face_of(3, depth - 1)], 50)
    up = shift(send, "lev", 1)
    send, *rest = take(
        view,
        low_row,
        [face, (4, width), (4, width), (4, depth), (4, depth)],
        [
            face_of(0, depth - 1),
            edge_of(lambda w, z: w.at[depth - 1, :, z]),
            edge_of(lambda w, z: w.at[0, :, z]),
            edge_of(lambda w, z: w.at[:, width - 1, z]),
            edge_of(lambda w, z: w.at[:, 0, z]),
        ],
        10,
    )
    sides = exchange(*rest)
    down = shift(send, "lev", -1)
    u, d, f = (split(a, (0, 1, 2, 3)) for a in (raw, d, f))
    order = (0, 1, 2, 3)
    for step in range(STEPS):
        where = [(sides, order.index(z)) for z in range(4)]
        rows = pick(sides, (order.index(3), order.index(0)), low_row)
        low, high = (up, relay(rows[0], 1)), (down, relay(rows[1], -1))
        if step == STEPS - 1:
            break
        first, second = (0, 3) if step % 2 == 0 else (3, 0)
        most = (first, 1, 2) if first == 0 else (3, 2, 1)
        made, carried = grow(most, low_row, u, low, high, d, f, where, False)
        early = shift(cut(made[0], 0, depth - 1, low_row), "lev", -1 if first == 0 else 1)
        (v,), rest = grow((second,), low_row, u, low, high, d, f, where, False, carried)
        sides = exchange(*rest)
        if step < STEPS - 2:
            late = shift(cut(v, 0, depth - 1, low_row), "lev", -1 if second == 0 else 1)
        else:
            late = [shift(cut(v, 0, CUT, low_row), "lev", 1)]
            late.append(shift(cut(v, CUT, depth - 1 - CUT, low_row), "lev", 1))
        order = most + (second,)
        made = dict(zip(order, [*made, v]))
        u = [made[z] for z in range(4)]
        up, down = (late, early) if first == 0 else (early, late)
    made, (stat,) = grow((3, 2, 1), low_row, u, low, high, d, f, where, True)
    stats = from_all(stat)
    filled = finish((3, 2, 1), made, stats)
    score, end = (x.reshape(depth, width, 4, 1, lanes) for x in filled)
    pieces, edge = low
    for name, start, stop in (("b", 0, CUT), ("c", CUT, depth)):
        near = pieces[:1] if name == "b" else pieces
        rows, stat = grow_last(start, stop - start, low_row, u, near, edge, d[0], f[0], where[0])
        stats = from_all(stat)
        end = put(end, rows, start)
        score = put_scaled(score, rows, stats, start)
    return score.reshape(initial_heat.shape), end.reshape(initial_heat.shape)


def solution(mesh):
    placed = P("lat", "lon", "lev", None)

    return jax.shard_map(
        local,
        mesh=mesh,
        in_specs=(placed,) * 3,
        out_specs=(placed, placed),
        check_vma=False,
    )
```
